32 devices in a mesh: seq: 16 (over z, y, x), head: 2 (over core).
Axes of the slice: x: 2, y: 2, z: 4, core: 2. Of those that a mesh axis runs over, the one named last changes fastest.
Arguments:
- queries: bfloat16 [2048, 2048], P('seq', 'head'), may hold values from -6 to 6
- keys: bfloat16 [2048, 512], P('seq', 'head'), may hold values from -6 to 6
- values: bfloat16 [2048, 512], P('seq', 'head'), may hold values from -6 to 6
- tile_mask: int32 [32, 32], replicated, may hold values from 0 to 1, as said below
- out_weight: bfloat16 [2048, 4096], P('head'), may hold values from -0.5 to 0.5
Outputs:
- mixed: bfloat16 [2048, 4096], P(('seq', 'head'))
The draws below stay inside these ranges and needn't reach their ends.
Inputs may be any that keep to these rules, and one draw needn't show every extreme that they name: tile_mask[i, j] is 1 for i == j, 0 for j > i, and 0 or 1 below the diagonal.
All inputs are finite; a program needn't handle non-finite values.
Results may differ from the reference program's by a relative error of at most 0.01.
Values may be sent and summed in bfloat16 or wider, within the bound.
A program may use at most 128 MiB of HBM per device.

```python
import math
import jax
import jax.numpy as jnp
from jax import lax

D = 4096
HD = 128
HEADS = 16
KVH = 4
TILE = 64
TOKENS = 2048
TILES = 32


def draw_field(key, salt, heads_count):
    base = jax.random.fold_in(key, salt)
    field = 1.5 * jax.random.truncated_normal(base, -4.0, 4.0, (TOKENS, heads_count * HD), jnp.float32)
    return field.astype(jnp.bfloat16)


def draw_queries(key, part):
    return draw_field(key, 1, HEADS)


def draw_keys(key, part):
    return draw_field(key, 2, KVH)


def draw_tile_mask(key, part):
    coin = jax.random.randint(jax.random.fold_in(key, 3), (TILES, TILES), 0, 2, dtype=jnp.int32)
    row_index = jnp.arange(TILES, dtype=jnp.int32)[:, None]
    column_index = jnp.arange(TILES, dtype=jnp.int32)[None, :]
    diagonal = jnp.where(row_index == column_index, 1, 0).astype(jnp.int32)
    return jnp.where(row_index > column_index, coin, diagonal).astype(jnp.int32)


def level_of(stream_key, dims, split, low, top_value):
    def one(axis_at, shards_of):
        heights = jax.random.uniform(jax.random.fold_in(jax.random.fold_in(stream_key, 6), axis_at), (shards_of,), jnp.float32, low / len(split), top_value / len(split))
        return jnp.repeat(jnp.exp(heights), dims[axis_at] // shards_of).reshape((-1,) + (1,) * (len(dims) - axis_at - 1))

    gain = one(*split[0])
    for cut in split[1:]:
        gain = gain * one(*cut)
    return gain


def scatter_about(stream_key, dims, deviation, reach, split=(), kind=jnp.bfloat16):
    result = deviation * jax.random.normal(stream_key, dims, jnp.float32)
    if split:
        result = result * level_of(stream_key, dims, split, -0.22, 0.18)
    return jnp.clip(result, -reach, reach).astype(kind)


def setup_inputs(seed: int = 0) -> dict:
    key_of = jax.random.split(jax.random.key(seed), 6)
    return {
        "queries": draw_queries(jax.random.fold_in(key_of[5], 71), 0),
        "keys": draw_keys(jax.random.fold_in(key_of[5], 71), 0),
        "values": scatter_about(key_of[2], (TOKENS, KVH * HD), 1.0, 6.0, ((0, 16), (1, 2))),
        "tile_mask": draw_tile_mask(jax.random.fold_in(key_of[5], 71), 0),
        "out_weight": scatter_about(key_of[4], (HEADS * HD, D), HD ** -0.5, 0.5, ((0, 2),)),
    }


MASK_FLOOR = -1e+30

def reference(queries, keys, values, tile_mask, out_weight):
    group = HEADS // KVH
    scale = 1.0 / math.sqrt(HD)
    query_field = queries.reshape(TOKENS, KVH, group, HD)
    key_field = keys.reshape(TOKENS, KVH, HD).astype(jnp.float32)
    value_field = values.reshape(TOKENS, KVH, HD).astype(jnp.float32)
    key_index = jnp.arange(TOKENS, dtype=jnp.int32)
    key_tile = key_index // TILE

    def one_tile(tile):
        row_start = (tile * TILE).astype(jnp.int32)
        query_tile = lax.dynamic_slice_in_dim(query_field, row_start, TILE, 0).astype(jnp.float32)
        query_index = row_start + jnp.arange(TILE, dtype=jnp.int32)
        mask_row = lax.dynamic_index_in_dim(tile_mask, tile, 0, keepdims=False)
        allowed = (mask_row[key_tile] > 0)[None, :] & (key_index[None, :] <= query_index[:, None])
        allowed_wide = allowed[:, None, None, :]
        scores = jnp.einsum('qgrd,kgd->qgrk', query_tile, key_field, precision=lax.Precision.HIGHEST) * scale
        masked = jnp.where(allowed_wide, scores, MASK_FLOOR)
        best = lax.optimization_barrier(jnp.max(masked, axis=-1, keepdims=True))
        weights = jnp.where(allowed_wide, jnp.exp(masked - best), 0.0)
        total = lax.optimization_barrier(jnp.sum(weights, axis=-1))
        rounded = lax.optimization_barrier(weights.astype(jnp.bfloat16)).astype(jnp.float32)
        blended = jnp.einsum('qgrk,kgd->qgrd', rounded, value_field, precision=lax.Precision.HIGHEST) / total[..., None]
        return blended.astype(jnp.bfloat16).reshape(TILE, HEADS * HD)
    attended = lax.map(one_tile, jnp.arange(TILES, dtype=jnp.int32)).reshape(TOKENS, HEADS * HD)
    return jnp.dot(attended, out_weight, preferred_element_type=jnp.float32).astype(jnp.bfloat16)
```

```python
import functools
import math

import jax
import jax.numpy as jnp
from jax import lax
from jax.experimental import pallas as pl
from jax.experimental.pallas import tpu as pltpu
from jax.sharding import PartitionSpec as P

HD = 128
MASK_FLOOR = -1e30
MESH = pl.DeviceIdType.MESH


def fused_kernel(
    dims,
    q_hbm, k_hbm, v_hbm, mask_ref, w_hbm,
    out_ref,
    q_in, kv_in, qbuf, kvbuf, wbuf, rowmask, best, acc, attbuf, abuf, part, sendbuf, rbuf,
    load_sem, w_sem, kv_send, kv_recv, q_send, q_recv, fwd_send, fwd_recv,
    a_send, a_recv, p_send, p_recv,
):
    planes, members, cores, local_groups, rows, heads, tile, blocks, width = dims
    place = lax.axis_index("seq")
    core = lax.axis_index("head")
    plane = place // members
    member = lax.rem(place, members)
    partner = 1 - core
    home = member // local_groups
    chunk = members * rows
    hw = heads * HD

    loads = [
        pltpu.make_async_copy(k_hbm, kv_in.at[0], load_sem.at[0]),
        pltpu.make_async_copy(v_hbm, kv_in.at[1], load_sem.at[1]),
        pltpu.make_async_copy(q_hbm, q_in, load_sem.at[2]),
    ]
    for load in loads:
        load.start()

    barrier = pltpu.get_barrier_semaphore()

    def greet(seq_to, head_to):
        pl.semaphore_signal(barrier, inc=1, device_id=(seq_to, head_to), device_id_type=MESH)

    for shift in range(members * cores):
        if shift == 0:
            continue
        other = lax.rem(member * cores + core + shift, members * cores)
        greet(plane * members + other // cores, lax.rem(other, cores))

    def greet_above(up, none):
        for l in range(local_groups):
            for kind in range(2):
                greet(up * members + core * local_groups + l, kind)
        return none

    def greet_below(down, none):
        for s in range(members):
            greet(down * members + s, home)
        return none

    lax.fori_loop(plane + 1, planes, greet_above, 0)
    lax.fori_loop(0, plane, greet_below, 0)

    w_copy = pltpu.make_async_copy(w_hbm, wbuf, w_sem)

    tiles = mask_ref.shape[0]
    row_at = plane * chunk + lax.broadcasted_iota(jnp.int32, (chunk, tiles), 0)
    tile_at = lax.broadcasted_iota(jnp.int32, (chunk, tiles), 1) * tile
    pick = jnp.where((row_at >= tile_at) & (row_at < tile_at + tile), 1.0, 0.0).astype(jnp.bfloat16)
    open_tiles = jnp.where(mask_ref[...] > 0, 1.0, 0.0).astype(jnp.bfloat16)
    rowmask[...] = jnp.dot(pick, open_tiles, preferred_element_type=jnp.float32).astype(jnp.bfloat16)

    for load in loads:
        load.wait()
    pl.semaphore_wait(barrier, members * cores - 1 + (planes - 1) * members)

    def kv_copy(up, l, kind):
        return pltpu.make_async_remote_copy(
            src_ref=kv_in.at[kind, :, pl.ds(l * HD, HD)],
            dst_ref=kvbuf.at[kind, pl.ds(pl.multiple_of(place * rows, rows), rows), :],
            send_sem=kv_send.at[up, l, kind],
            recv_sem=kv_recv.at[place],
            device_id=(up * members + core * local_groups + l, kind),
            device_id_type=MESH,
        )

    def send_above(step, none):
        up = planes - 1 - step
        for l in range(local_groups):
            for kind in range(2):
                kv_copy(up, l, kind).start()
        return none

    lax.fori_loop(0, planes - 1 - plane, send_above, 0)

    def kv_is_own(l, kind):
        return (core * local_groups + l == member) & (core == kind)

    for l in range(local_groups):
        for kind in range(2):
            own = kv_is_own(l, kind)

            @pl.when(own)
            def _():
                pltpu.make_async_copy(
                    kv_in.at[kind, :, pl.ds(l * HD, HD)],
                    kvbuf.at[kind, pl.ds(pl.multiple_of(place * rows, rows), rows), :],
                    kv_recv.at[place],
                ).start()

            @pl.when(jnp.logical_not(own))
            def _():
                kv_copy(plane, l, kind).start()

    def q_copy(l, e):
        return pltpu.make_async_remote_copy(
            src_ref=q_in.at[:, pl.ds((l * cores + e) * hw, hw)],
            dst_ref=qbuf.at[member],
            send_sem=q_send.at[l, e],
            recv_sem=q_recv.at[member],
            device_id=(plane * members + core * local_groups + l, e),
            device_id_type=MESH,
        )

    for l in range(local_groups):
        for e in range(cores):
            own = kv_is_own(l, e)

            @pl.when(own)
            def _():
                pltpu.make_async_copy(
                    q_in.at[:, pl.ds((l * cores + e) * hw, hw)], qbuf.at[member], q_recv.at[member]
                ).start()

            @pl.when(jnp.logical_not(own))
            def _():
                q_copy(l, e).start()

    w_copy.start()

    def fwd_copy(kc):
        where = pl.ds(pl.multiple_of(kc * chunk, chunk), chunk)
        return pltpu.make_async_remote_copy(
            src_ref=kvbuf.at[core, where, :],
            dst_ref=kvbuf.at[core, where, :],
            send_sem=fwd_send.at[kc],
            recv_sem=fwd_recv.at[kc],
            device_id=(place, partner),
            device_id_type=MESH,
        )

    def arrive(kc):
        for s in range(members):
            block = kvbuf.at[core, pl.ds(pl.multiple_of((kc * members + s) * rows, rows), rows), :]
            pltpu.make_async_copy(block, block, kv_recv.at[kc * members + s]).wait()
        fwd_copy(kc).start()

    def fwd_arrived(kc):
        block = kvbuf.at[partner, pl.ds(pl.multiple_of(kc * chunk, chunk), chunk), :]
        pltpu.make_async_copy(block, block, fwd_recv.at[kc]).wait()

    unit = math.log2(math.e) / math.sqrt(HD)

    def attend(kc, s, first):
        keys_here = (s + 1) * rows if first else chunk
        base = pl.multiple_of(kc * chunk, chunk)
        key_at = base + lax.broadcasted_iota(jnp.int32, (tiles, keys_here), 1)
        tile_from = lax.broadcasted_iota(jnp.int32, (tiles, keys_here), 0) * tile
        spread = jnp.where((key_at >= tile_from) & (key_at < tile_from + tile), 1.0, 0.0)
        opened = jnp.dot(
            rowmask[pl.ds(s * rows, rows), :],
            spread.astype(jnp.bfloat16),
            preferred_element_type=jnp.float32,
        )
        if first:
            r = s * rows + lax.broadcasted_iota(jnp.int32, (rows, keys_here), 0)
            u = lax.broadcasted_iota(jnp.int32, (rows, keys_here), 1)
            opened = jnp.where(u <= r, opened, 0.0)
        visible = opened > 0.5
        k_part = kvbuf[0, pl.ds(base, keys_here), :]
        v_part = kvbuf[1, pl.ds(base, keys_here), :]
        v_wide = jnp.concatenate([v_part, jnp.ones_like(v_part)], axis=1)
        for h in range(heads):
            scores = lax.dot_general(
                qbuf[s, :, h * HD : (h + 1) * HD],
                k_part,
                (((1,), (1,)), ((), ())),
                preferred_element_type=jnp.float32,
            )
            scores = jnp.where(visible, scores * unit, MASK_FLOOR)
            top = jnp.max(scores, axis=1, keepdims=True)
            if not first:
                before = best[h, s]
                top = jnp.maximum(before, top)
            weights = jnp.exp2(scores - top).astype(jnp.bfloat16)
            product = jnp.dot(weights, v_wide, preferred_element_type=jnp.float32)
            if not first:
                product = acc[h, s] * jnp.exp2(before - top) + product
            best[h, s] = top
            acc[h, s] = product

    arrive(plane)
    for s in range(members):
        block = qbuf.at[s]
        pltpu.make_async_copy(block, block, q_recv.at[s]).wait()
    fwd_arrived(plane)
    for s in range(members):
        attend(plane, s, True)

    def below(step, none):
        kc = plane - 1 - step
        arrive(kc)
        fwd_arrived(kc)
        for s in range(members):
            attend(kc, s, False)
        return none

    lax.fori_loop(0, plane, below, 0)

    slot = lax.rem(member, local_groups) * cores + core

    def a_copy(s):
        return pltpu.make_async_remote_copy(
            src_ref=attbuf.at[s],
            dst_ref=abuf.at[slot],
            send_sem=a_send.at[s],
            recv_sem=a_recv.at[slot],
            device_id=(plane * members + s, home),
            device_id_type=MESH,
        )

    def a_is_own(s):
        return (member == s) & (core == home)

    for s in range(members):
        for h in range(heads):
            total = acc[h, s]
            attbuf[s, :, h * HD : (h + 1) * HD] = (total[:, :HD] / total[:, HD:]).astype(jnp.bfloat16)

        @pl.when(a_is_own(s))
        def _():
            pltpu.make_async_copy(attbuf.at[s], abuf.at[slot], a_recv.at[slot]).start()

        @pl.when(jnp.logical_not(a_is_own(s)))
        def _():
            a_copy(s).start()

    w_copy.wait()
    for j in range(local_groups * cores):
        block = abuf.at[j]
        pltpu.make_async_copy(block, block, a_recv.at[j]).wait()

    half = rows // cores
    attended = jnp.concatenate([abuf[j] for j in range(local_groups * cores)], axis=1)

    def p_copy(j):
        return pltpu.make_async_remote_copy(
            src_ref=sendbuf.at[j, pl.ds(pl.multiple_of(partner * half, half), half), :],
            dst_ref=rbuf.at[j],
            send_sem=p_send.at[j],
            recv_sem=p_recv.at[j],
            device_id=(place, partner),
            device_id_type=MESH,
        )

    for j in range(blocks):
        product = jnp.dot(
            attended, wbuf[:, j * width : (j + 1) * width], preferred_element_type=jnp.float32
        )
        sendbuf[j] = product.astype(jnp.bfloat16)
        p_copy(j).start()
        part[j] = product
    for j in range(blocks):
        p_copy(j).wait_recv()
        mine = part[j, pl.ds(pl.multiple_of(core * half, half), half), :]
        out_ref[:, j * width : (j + 1) * width] = (mine + rbuf[j].astype(jnp.float32)).astype(
            out_ref.dtype
        )

    for j in range(blocks):
        p_copy(j).wait_send()
    for s in range(members):

        @pl.when(jnp.logical_not(a_is_own(s)))
        def _():
            a_copy(s).wait_send()

    for l in range(local_groups):
        for e in range(cores):

            @pl.when(jnp.logical_not(kv_is_own(l, e)))
            def _():
                q_copy(l, e).wait_send()
                kv_copy(plane, l, e).wait_send()

    def drain_above(step, none):
        up = planes - 1 - step
        for l in range(local_groups):
            for kind in range(2):
                kv_copy(up, l, kind).wait_send()
        return none

    lax.fori_loop(0, planes - 1 - plane, drain_above, 0)

    def drain_fwd(kc, none):
        fwd_copy(kc).wait_send()
        return none

    lax.fori_loop(0, plane + 1, drain_fwd, 0)


def per_device(sizes, queries, keys, values, tile_mask, out_weight):
    seq_size, cores = sizes
    rows = queries.shape[0]
    local_groups = keys.shape[1] // HD
    group = queries.shape[1] // HD // local_groups
    members = local_groups * cores
    planes = seq_size // members
    heads = group // cores
    tile = rows * seq_size // tile_mask.shape[0]
    columns = out_weight.shape[1]
    width = math.gcd(columns, 512)
    blocks = columns // width
    dims = (planes, members, cores, local_groups, rows, heads, tile, blocks, width)
    bf16, f32 = jnp.bfloat16, jnp.float32
    DMA = pltpu.SemaphoreType.DMA
    any_spec = pl.BlockSpec(memory_space=pl.ANY)
    vmem_spec = pl.BlockSpec(memory_space=pltpu.VMEM)
    return pl.pallas_call(
        functools.partial(fused_kernel, dims),
        out_shape=jax.ShapeDtypeStruct((rows // cores, columns), bf16),
        in_specs=[any_spec, any_spec, any_spec, vmem_spec, any_spec],
        out_specs=vmem_spec,
        scratch_shapes=[
            pltpu.VMEM(queries.shape, bf16),
            pltpu.VMEM((2,) + keys.shape, bf16),
            pltpu.VMEM((members, rows, heads * HD), bf16),
            pltpu.VMEM((2, seq_size * rows, HD), bf16),
            pltpu.VMEM(out_weight.shape, bf16),
            pltpu.VMEM((members * rows, tile_mask.shape[0]), bf16),
            pltpu.VMEM((heads, members, rows, 1), f32),
            pltpu.VMEM((heads, members, rows, 2 * HD), f32),
            pltpu.VMEM((members, rows, heads * HD), bf16),
            pltpu.VMEM((members, rows, heads * HD), bf16),
            pltpu.VMEM((blocks, rows, width), f32),
            pltpu.VMEM((blocks, rows, width), bf16),
            pltpu.VMEM((blocks, rows // cores, width), bf16),
            DMA((3,)),
            DMA,
            DMA((planes, local_groups, 2)),
            DMA((seq_size,)),
            DMA((local_groups, cores)),
            DMA((members,)),
            DMA((planes,)),
            DMA((planes,)),
            DMA((members,)),
            DMA((members,)),
            DMA((blocks,)),
            DMA((blocks,)),
        ],
        compiler_params=pltpu.CompilerParams(
            collective_id=0, has_side_effects=True, vmem_limit_bytes=60 * 1024 * 1024
        ),
        name="attend_project",
    )(queries, keys, values, tile_mask, out_weight)


def solution(mesh):
    placed = (P("seq", "head"), P("seq", "head"), P("seq", "head"), P(), P("head", None))
    sizes = (mesh.shape["seq"], mesh.shape["head"])
    return jax.shard_map(
        functools.partial(per_device, sizes),
        mesh=mesh,
        in_specs=placed,
        out_specs=P(("seq", "head"), None),
        check_vma=False,
    )
```

```python
import functools
import math

import jax
import jax.numpy as jnp
from jax import lax
from jax.experimental import pallas as pl
from jax.experimental.pallas import tpu as pltpu
from jax.sharding import PartitionSpec as P

HD = 128
MASK_FLOOR = -1e30
MESH = pl.DeviceIdType.MESH


def fused_kernel(
    dims,
    q_hbm, k_hbm, v_hbm, mask_ref, w_hbm,
    out_ref,
    q_in, kv_in, qbuf, qext, kvbuf, spread, wbuf, best, acc, attbuf, abuf, part, sendbuf, rbuf,
    load_sem, w_sem, kv_send, kv_recv, q_send, q_recv, z_send, fwd_send, fwd_recv,
    a_send, a_recv, p_send, p_recv,
):
    planes, members, cores, local_groups, rows, heads, tile, blocks, width = dims
    place = lax.axis_index("seq")
    core = lax.axis_index("head")
    plane = place // members
    member = lax.rem(place, members)
    partner = 1 - core
    home = member // local_groups
    chunk = members * rows
    hw = heads * HD

    loads = [
        pltpu.make_async_copy(k_hbm, kv_in.at[0], load_sem.at[0]),
        pltpu.make_async_copy(v_hbm, kv_in.at[1], load_sem.at[1]),
        pltpu.make_async_copy(q_hbm, q_in, load_sem.at[2]),
    ]
    for load in loads:
        load.start()

    barrier = pltpu.get_barrier_semaphore()

    def greet(seq_to, head_to):
        pl.semaphore_signal(barrier, inc=1, device_id=(seq_to, head_to), device_id_type=MESH)

    for shift in range(1, members * cores):
        other = lax.rem(member * cores + core + shift, members * cores)
        greet(plane * members + other // cores, lax.rem(other, cores))

    @pl.when(plane < planes - 1)
    def _():
        greet(place + members, core)

    @pl.when(plane > 0)
    def _():
        greet(place - members, core)

    w_copy = pltpu.make_async_copy(w_hbm, wbuf, w_sem)

    tiles = mask_ref.shape[0]
    wide = qext.shape[2] - HD
    row_at = plane * chunk + lax.broadcasted_iota(jnp.int32, (chunk, tiles), 0)
    tile_at = lax.broadcasted_iota(jnp.int32, (chunk, tiles), 1) * tile
    pick = jnp.where((row_at >= tile_at) & (row_at < tile_at + tile), 1.0, 0.0).astype(jnp.bfloat16)
    closed = jnp.where(mask_ref[...] > 0, 0.0, 1.0).astype(jnp.bfloat16)
    if wide > tiles:
        closed = jnp.concatenate([closed, jnp.zeros((tiles, wide - tiles), jnp.bfloat16)], axis=1)
    shut = jnp.dot(pick, closed, preferred_element_type=jnp.float32)
    floor = jnp.where(shut > 0.5, MASK_FLOOR, 0.0).astype(jnp.bfloat16)
    for s in range(members):
        for h in range(heads):
            qext[s, h * rows : (h + 1) * rows, HD:] = floor[s * rows : (s + 1) * rows, :]

    for load in loads:
        load.wait()
    pl.semaphore_wait(
        barrier,
        members * cores - 1 + jnp.minimum(plane, 1) + jnp.minimum(planes - 1 - plane, 1),
    )

    def is_own(l, kind):
        return (core * local_groups + l == member) & (core == kind)

    def block_at(index):
        return pl.ds(pl.multiple_of(index * rows, rows), rows)

    def kv_copy(l, kind):
        return pltpu.make_async_remote_copy(
            src_ref=kv_in.at[kind, :, pl.ds(l * HD, HD)],
            dst_ref=kvbuf.at[kind, block_at(place), :],
            send_sem=kv_send.at[l, kind],
            recv_sem=kv_recv.at[place],
            device_id=(plane * members + core * local_groups + l, kind),
            device_id_type=MESH,
        )

    for l in range(local_groups):
        for kind in range(2):

            @pl.when(is_own(l, kind))
            def _():
                pltpu.make_async_copy(
                    kv_in.at[kind, :, pl.ds(l * HD, HD)],
                    kvbuf.at[kind, block_at(place), :],
                    kv_recv.at[place],
                ).start()

            @pl.when(jnp.logical_not(is_own(l, kind)))
            def _():
                kv_copy(l, kind).start()

    def q_copy(l, e):
        return pltpu.make_async_remote_copy(
            src_ref=q_in.at[:, pl.ds((l * cores + e) * hw, hw)],
            dst_ref=qbuf.at[member],
            send_sem=q_send.at[l, e],
            recv_sem=q_recv.at[member],
            device_id=(plane * members + core * local_groups + l, e),
            device_id_type=MESH,
        )

    for l in range(local_groups):
        for e in range(cores):

            @pl.when(is_own(l, e))
            def _():
                pltpu.make_async_copy(
                    q_in.at[:, pl.ds((l * cores + e) * hw, hw)], qbuf.at[member], q_recv.at[member]
                ).start()

            @pl.when(jnp.logical_not(is_own(l, e)))
            def _():
                q_copy(l, e).start()

    w_copy.start()

    def z_copy(index):
        return pltpu.make_async_remote_copy(
            src_ref=kvbuf.at[core, block_at(index), :],
            dst_ref=kvbuf.at[core, block_at(index), :],
            send_sem=z_send.at[index],
            recv_sem=kv_recv.at[index],
            device_id=(place + members, core),
            device_id_type=MESH,
        )

    def fwd_copy(index):
        return pltpu.make_async_remote_copy(
            src_ref=kvbuf.at[core, block_at(index), :],
            dst_ref=kvbuf.at[core, block_at(index), :],
            send_sem=fwd_send.at[index],
            recv_sem=fwd_recv.at[index],
            device_id=(place, partner),
            device_id_type=MESH,
        )

    def relay(kc, turn):
        across = lax.rem(member // 2 + turn // 2, members // 2) * 2
        index = kc * members + across + lax.rem(lax.rem(member, 2) + turn % 2, 2)
        block = kvbuf.at[core, block_at(index), :]
        pltpu.make_async_copy(block, block, kv_recv.at[index]).wait()

        @pl.when(plane < planes - 1)
        def _():
            z_copy(index).start()

        fwd_copy(index).start()

    def settle(kc):
        for s in range(members):
            block = kvbuf.at[partner, block_at(kc * members + s), :]
            pltpu.make_async_copy(block, block, fwd_recv.at[kc * members + s]).wait()
        key_at = kc * chunk + lax.broadcasted_iota(jnp.int32, (chunk, wide), 0)
        tile_from = lax.broadcasted_iota(jnp.int32, (chunk, wide), 1) * tile
        inside = (key_at >= tile_from) & (key_at < tile_from + tile)
        spread[...] = jnp.where(inside, 1.0, 0.0).astype(jnp.bfloat16)

    unit = math.log2(math.e) / math.sqrt(HD)

    def attend(kc, s, first):
        keys_here = (s + 1) * rows if first else chunk
        base = pl.multiple_of(kc * chunk, chunk)
        k_wide = jnp.concatenate([kvbuf[0, pl.ds(base, keys_here), :], spread[:keys_here, :]], axis=1)
        v_part = kvbuf[1, pl.ds(base, keys_here), :]
        v_wide = jnp.concatenate([v_part, jnp.ones_like(v_part)], axis=1)
        scores = lax.dot_general(
            qext[s], k_wide, (((1,), (1,)), ((), ())), preferred_element_type=jnp.float32
        )
        if first:
            r = s * rows + lax.broadcasted_iota(jnp.int32, (rows, keys_here), 0)
            u = lax.broadcasted_iota(jnp.int32, (rows, keys_here), 1)
            later = jnp.where(u <= r, 0.0, MASK_FLOOR)
            scores = scores + jnp.concatenate([later] * heads, axis=0)
        top = jnp.max(scores, axis=1, keepdims=True)
        if not first:
            before = best[s]
            top = jnp.maximum(before, top)
        weights = jnp.exp2((scores - top) * unit).astype(jnp.bfloat16)
        product = jnp.dot(weights, v_wide, preferred_element_type=jnp.float32)
        if not first:
            product = acc[s] * jnp.exp2((before - top) * unit) + product
        best[s] = top
        acc[s] = product

    slot = lax.rem(member, local_groups) * cores + core

    def a_copy(s):
        return pltpu.make_async_remote_copy(
            src_ref=attbuf.at[s],
            dst_ref=abuf.at[slot],
            send_sem=a_send.at[s],
            recv_sem=a_recv.at[slot],
            device_id=(plane * members + s, home),
            device_id_type=MESH,
        )

    def a_is_own(s):
        return (member == s) & (core == home)

    def give_back(s):
        for h in range(heads):
            total = acc[s, h * rows : (h + 1) * rows, :]
            attbuf[s, :, h * HD : (h + 1) * HD] = (total[:, :HD] / total[:, HD:]).astype(jnp.bfloat16)

        @pl.when(a_is_own(s))
        def _():
            pltpu.make_async_copy(attbuf.at[s], abuf.at[slot], a_recv.at[slot]).start()

        @pl.when(jnp.logical_not(a_is_own(s)))
        def _():
            a_copy(s).start()

    for t in range(members):
        relay(plane, t)

    @pl.when(plane >= 1)
    def _():
        for t in range(members):
            relay(plane - 1, t)

    settle(plane)
    for s in range(members):

        @pl.when(plane >= 2)
        def _():
            relay(plane - 2, s)

        block = qbuf.at[s]
        pltpu.make_async_copy(block, block, q_recv.at[s]).wait()
        for h in range(heads):
            qext[s, h * rows : (h + 1) * rows, :HD] = qbuf[s, :, h * HD : (h + 1) * HD]
        attend(plane, s, True)

    def below(step, none):
        settle(plane - step)
        for s in range(members):

            @pl.when(step + 2 <= plane)
            def _():
                relay(plane - step - 2, s)

            attend(plane - step, s, False)
        return none

    lax.fori_loop(1, plane, below, 0)

    @pl.when(plane >= 1)
    def _():
        settle(0)
        for s in range(members):
            attend(0, s, False)
            give_back(s)

    @pl.when(plane == 0)
    def _():
        for s in range(members):
            give_back(s)

    w_copy.wait()
    for j in range(local_groups * cores):
        block = abuf.at[j]
        pltpu.make_async_copy(block, block, a_recv.at[j]).wait()

    half = rows // cores
    attended = jnp.concatenate([abuf[j] for j in range(local_groups * cores)], axis=1)

    def p_copy(j):
        return pltpu.make_async_remote_copy(
            src_ref=sendbuf.at[j, pl.ds(pl.multiple_of(partner * half, half), half), :],
            dst_ref=rbuf.at[j],
            send_sem=p_send.at[j],
            recv_sem=p_recv.at[j],
            device_id=(place, partner),
            device_id_type=MESH,
        )

    for j in range(blocks):
        product = jnp.dot(
            attended, wbuf[:, j * width : (j + 1) * width], preferred_element_type=jnp.float32
        )
        sendbuf[j] = product.astype(jnp.bfloat16)
        p_copy(j).start()
        part[j] = product
    for j in range(blocks):
        p_copy(j).wait_recv()
        mine = part[j, pl.ds(pl.multiple_of(core * half, half), half), :]
        out_ref[:, j * width : (j + 1) * width] = (mine + rbuf[j].astype(jnp.float32)).astype(
            out_ref.dtype
        )

    for j in range(blocks):
        p_copy(j).wait_send()
    for s in range(members):

        @pl.when(jnp.logical_not(a_is_own(s)))
        def _():
            a_copy(s).wait_send()

    for l in range(local_groups):
        for e in range(cores):

            @pl.when(jnp.logical_not(is_own(l, e)))
            def _():
                q_copy(l, e).wait_send()
                kv_copy(l, e).wait_send()

    def drain(index, none):
        fwd_copy(index).wait_send()

        @pl.when(plane < planes - 1)
        def _():
            z_copy(index).wait_send()

        return none

    lax.fori_loop(0, (plane + 1) * members, drain, 0)


def per_device(sizes, queries, keys, values, tile_mask, out_weight):
    seq_size, cores = sizes
    rows = queries.shape[0]
    local_groups = keys.shape[1] // HD
    group = queries.shape[1] // HD // local_groups
    members = local_groups * cores
    planes = seq_size // members
    heads = group // cores
    tile = rows * seq_size // tile_mask.shape[0]
    columns = out_weight.shape[1]
    wide = -(-tile_mask.shape[0] // HD) * HD
    width = math.gcd(columns, 512)
    blocks = columns // width
    dims = (planes, members, cores, local_groups, rows, heads, tile, blocks, width)
    bf16, f32 = jnp.bfloat16, jnp.float32
    DMA = pltpu.SemaphoreType.DMA
    any_spec = pl.BlockSpec(memory_space=pl.ANY)
    vmem_spec = pl.BlockSpec(memory_space=pltpu.VMEM)
    return pl.pallas_call(
        functools.partial(fused_kernel, dims),
        out_shape=jax.ShapeDtypeStruct((rows // cores, columns), bf16),
        in_specs=[any_spec, any_spec, any_spec, vmem_spec, any_spec],
        out_specs=vmem_spec,
        scratch_shapes=[
            pltpu.VMEM(queries.shape, bf16),
            pltpu.VMEM((2,) + keys.shape, bf16),
            pltpu.VMEM((members, rows, heads * HD), bf16),
            pltpu.VMEM((members, heads * rows, HD + wide), bf16),
            pltpu.VMEM((2, seq_size * rows, HD), bf16),
            pltpu.VMEM((members * rows, wide), bf16),
            pltpu.VMEM(out_weight.shape, bf16),
            pltpu.VMEM((members, heads * rows, 1), f32),
            pltpu.VMEM((members, heads * rows, 2 * HD), f32),
            pltpu.VMEM((members, rows, heads * HD), bf16),
            pltpu.VMEM((members, rows, heads * HD), bf16),
            pltpu.VMEM((blocks, rows, width), f32),
            pltpu.VMEM((blocks, rows, width), bf16),
            pltpu.VMEM((blocks, rows // cores, width), bf16),
            DMA((3,)),
            DMA,
            DMA((local_groups, 2)),
            DMA((seq_size,)),
            DMA((local_groups, cores)),
            DMA((members,)),
            DMA((seq_size,)),
            DMA((seq_size,)),
            DMA((seq_size,)),
            DMA((members,)),
            DMA((members,)),
            DMA((blocks,)),
            DMA((blocks,)),
        ],
        compiler_params=pltpu.CompilerParams(
            collective_id=0, has_side_effects=True, vmem_limit_bytes=60 * 1024 * 1024
        ),
        name="attend_project",
    )(queries, keys, values, tile_mask, out_weight)


def solution(mesh):
    placed = (P("seq", "head"), P("seq", "head"), P("seq", "head"), P(), P("head", None))
    sizes = (mesh.shape["seq"], mesh.shape["head"])
    return jax.shard_map(
        functools.partial(per_device, sizes),
        mesh=mesh,
        in_specs=placed,
        out_specs=P(("seq", "head"), None),
        check_vma=False,
    )
```

```python
import functools
import math

import jax
import jax.numpy as jnp
from jax import lax
from jax.experimental import pallas as pl
from jax.experimental.pallas import tpu as pltpu
from jax.sharding import PartitionSpec as P

HD = 128
MASK_FLOOR = -1e30
MESH = pl.DeviceIdType.MESH


def fused_kernel(
    dims,
    q_hbm, k_hbm, v_hbm, mask_hbm, w_hbm,
    out_ref,
    mask_ref, q_in, kv_in, qbuf, qext, kvbuf, spread, wbuf, best, acc, attbuf, abuf, part, sendbuf, rbuf,
    load_sem, w_sem, kv_send, kv_recv, q_send, q_recv, z_send, fwd_send, fwd_recv,
    a_send, a_recv, p_send, p_recv,
):
    planes, members, cores, local_groups, rows, heads, tile, blocks, width = dims
    place = lax.axis_index("seq")
    core = lax.axis_index("head")
    plane = place // members
    member = lax.rem(place, members)
    partner = 1 - core
    home = member // local_groups
    chunk = members * rows
    hw = heads * HD

    loads = [
        pltpu.make_async_copy(k_hbm, kv_in.at[0], load_sem.at[0]),
        pltpu.make_async_copy(v_hbm, kv_in.at[1], load_sem.at[1]),
        pltpu.make_async_copy(q_hbm, q_in, load_sem.at[2]),
        pltpu.make_async_copy(mask_hbm, mask_ref, load_sem.at[3]),
    ]
    for load in loads:
        load.start()

    barrier = pltpu.get_barrier_semaphore()

    def greet(seq_to, head_to):
        pl.semaphore_signal(barrier, inc=1, device_id=(seq_to, head_to), device_id_type=MESH)

    for shift in range(1, members * cores):
        peer = lax.rem(member * cores + core + shift, members * cores)
        greet(plane * members + peer // cores, lax.rem(peer, cores))

    @pl.when(plane < planes - 1)
    def _():
        greet(place + members, core)

    @pl.when(plane > 0)
    def _():
        greet(place - members, core)

    w_copy = pltpu.make_async_copy(w_hbm, wbuf, w_sem)

    for load in loads[:2]:
        load.wait()
    pl.semaphore_wait(
        barrier,
        members * cores - 1 + jnp.minimum(plane, 1) + jnp.minimum(planes - 1 - plane, 1),
    )

    def is_own(l, kind):
        return (core * local_groups + l == member) & (core == kind)

    def block_at(index):
        return pl.ds(pl.multiple_of(index * rows, rows), rows)

    def kv_copy(l, kind):
        return pltpu.make_async_remote_copy(
            src_ref=kv_in.at[kind, :, pl.ds(l * HD, HD)],
            dst_ref=kvbuf.at[kind, block_at(place), :],
            send_sem=kv_send.at[l, kind],
            recv_sem=kv_recv.at[place],
            device_id=(plane * members + core * local_groups + l, kind),
            device_id_type=MESH,
        )

    for l in range(local_groups):
        for kind in range(2):

            @pl.when(is_own(l, kind))
            def _():
                pltpu.make_async_copy(
                    kv_in.at[kind, :, pl.ds(l * HD, HD)],
                    kvbuf.at[kind, block_at(place), :],
                    kv_recv.at[place],
                ).start()

            @pl.when(jnp.logical_not(is_own(l, kind)))
            def _():
                kv_copy(l, kind).start()

    for load in loads[2:]:
        load.wait()

    def q_copy(l, e):
        return pltpu.make_async_remote_copy(
            src_ref=q_in.at[:, pl.ds((l * cores + e) * hw, hw)],
            dst_ref=qbuf.at[member],
            send_sem=q_send.at[l, e],
            recv_sem=q_recv.at[member],
            device_id=(plane * members + core * local_groups + l, e),
            device_id_type=MESH,
        )

    for l in range(local_groups):
        for e in range(cores):

            @pl.when(is_own(l, e))
            def _():
                pltpu.make_async_copy(
                    q_in.at[:, pl.ds((l * cores + e) * hw, hw)], qbuf.at[member], q_recv.at[member]
                ).start()

            @pl.when(jnp.logical_not(is_own(l, e)))
            def _():
                q_copy(l, e).start()

    w_copy.start()

    def z_copy(index):
        return pltpu.make_async_remote_copy(
            src_ref=kvbuf.at[core, block_at(index), :],
            dst_ref=kvbuf.at[core, block_at(index), :],
            send_sem=z_send.at[index],
            recv_sem=kv_recv.at[index],
            device_id=(place + members, core),
            device_id_type=MESH,
        )

    def fwd_copy(index):
        return pltpu.make_async_remote_copy(
            src_ref=kvbuf.at[core, block_at(index), :],
            dst_ref=kvbuf.at[core, block_at(index), :],
            send_sem=fwd_send.at[index],
            recv_sem=fwd_recv.at[index],
            device_id=(place, partner),
            device_id_type=MESH,
        )

    def other(turn):
        across = lax.rem(member // 2 + turn // 2, members // 2) * 2
        return across + lax.rem(lax.rem(member, 2) + turn % 2, 2)

    def relay(kc, turn):
        index = kc * members + other(turn)
        block = kvbuf.at[core, block_at(index), :]
        pltpu.make_async_copy(block, block, kv_recv.at[index]).wait()

        @pl.when(plane < planes - 1)
        def _():
            z_copy(index).start()

        fwd_copy(index).start()

    def settle(kc):
        for s in range(members):
            block = kvbuf.at[partner, block_at(kc * members + s), :]
            pltpu.make_async_copy(block, block, fwd_recv.at[kc * members + s]).wait()
        key_at = kc * chunk + lax.broadcasted_iota(jnp.int32, (chunk, wide), 0)
        tile_from = lax.broadcasted_iota(jnp.int32, (chunk, wide), 1) * tile
        inside = (key_at >= tile_from) & (key_at < tile_from + tile)
        spread[...] = jnp.where(inside, 1.0, 0.0).astype(jnp.bfloat16)

    unit = math.log2(math.e) / math.sqrt(HD)

    def attend(kc, parts, first):
        base = pl.multiple_of(kc * chunk, chunk)
        olds = [None if first else (best[s], acc[s]) for s in parts]
        news = []
        for s, old in zip(parts, olds):
            keys_here = (s + 1) * rows if first else chunk
            k_part = kvbuf[0, pl.ds(base, keys_here), :]
            k_wide = jnp.concatenate([k_part, spread[:keys_here, :]], axis=1)
            v_part = kvbuf[1, pl.ds(base, keys_here), :]
            v_wide = jnp.concatenate([v_part, jnp.ones_like(v_part)], axis=1)
            scores = lax.dot_general(
                qext[s], k_wide, (((1,), (1,)), ((), ())), preferred_element_type=jnp.float32
            )
            if first:
                r = s * rows + lax.broadcasted_iota(jnp.int32, (rows, keys_here), 0)
                u = lax.broadcasted_iota(jnp.int32, (rows, keys_here), 1)
                later = jnp.where(u <= r, 0.0, MASK_FLOOR)
                scores = scores + jnp.concatenate([later] * heads, axis=0)
            top = jnp.max(scores, axis=1, keepdims=True)
            if not first:
                top = jnp.maximum(old[0], top)
            weights = jnp.exp2((scores - top) * unit).astype(jnp.bfloat16)
            product = jnp.dot(weights, v_wide, preferred_element_type=jnp.float32)
            if not first:
                product = old[1] * jnp.exp2((old[0] - top) * unit) + product
            news.append((top, product))
        for s, new in zip(parts, news):
            best[s] = new[0]
            acc[s] = new[1]
        return news

    slot = lax.rem(member, local_groups) * cores + core

    def a_copy(s):
        return pltpu.make_async_remote_copy(
            src_ref=attbuf.at[s],
            dst_ref=abuf.at[slot],
            send_sem=a_send.at[s],
            recv_sem=a_recv.at[slot],
            device_id=(plane * members + s, home),
            device_id_type=MESH,
        )

    def a_is_own(s):
        return (member == s) & (core == home)

    def give_back(s, total):
        for h in range(heads):
            mine = total[h * rows : (h + 1) * rows, :]
            attbuf[s, :, h * HD : (h + 1) * HD] = (mine[:, :HD] / mine[:, HD:]).astype(jnp.bfloat16)

        @pl.when(a_is_own(s))
        def _():
            pltpu.make_async_copy(attbuf.at[s], abuf.at[slot], a_recv.at[slot]).start()

        @pl.when(jnp.logical_not(a_is_own(s)))
        def _():
            a_copy(s).start()

    for t in range(members):
        relay(plane, t)

    @pl.when(plane >= 1)
    def _():
        for t in range(members):
            relay(plane - 1, t)

    tiles = mask_ref.shape[0]
    wide = qext.shape[2] - HD
    row_at = plane * chunk + lax.broadcasted_iota(jnp.int32, (chunk, tiles), 0)
    tile_at = lax.broadcasted_iota(jnp.int32, (chunk, tiles), 1) * tile
    pick = jnp.where((row_at >= tile_at) & (row_at < tile_at + tile), 1.0, 0.0).astype(jnp.bfloat16)
    closed = jnp.where(mask_ref[...] > 0, 0.0, 1.0).astype(jnp.bfloat16)
    if wide > tiles:
        closed = jnp.concatenate([closed, jnp.zeros((tiles, wide - tiles), jnp.bfloat16)], axis=1)
    shut = jnp.dot(pick, closed, preferred_element_type=jnp.float32)
    floor = jnp.where(shut > 0.5, MASK_FLOOR, 0.0).astype(jnp.bfloat16)
    for s in range(members):
        for h in range(heads):
            qext[s, h * rows : (h + 1) * rows, HD:] = floor[s * rows : (s + 1) * rows, :]

    settle(plane)
    for pair in range(0, members, 2):

        @pl.when(plane >= 2)
        def _():
            relay(plane - 2, pair)
            relay(plane - 2, pair + 1)

        for s in (pair, pair + 1):
            block = qbuf.at[s]
            pltpu.make_async_copy(block, block, q_recv.at[s]).wait()
            for h in range(heads):
                qext[s, h * rows : (h + 1) * rows, :HD] = qbuf[s, :, h * HD : (h + 1) * HD]
        attend(plane, (pair, pair + 1), True)

    def below(step, none):
        settle(plane - step)
        for pair in range(0, members, 2):

            @pl.when(step + 2 <= plane)
            def _():
                relay(plane - step - 2, pair)
                relay(plane - step - 2, pair + 1)

            attend(plane - step, (pair, pair + 1), False)
        return none

    lax.fori_loop(1, plane, below, 0)

    @pl.when(plane >= 1)
    def _():
        settle(0)
        for pair in range(members // 2 - 1, -1, -1):
            parts = (other(2 * pair + 1), other(2 * pair))
            news = attend(0, parts, False)
            for s, new in zip(parts, news):
                give_back(s, new[1])

    @pl.when(plane == 0)
    def _():
        for turn in range(members - 1, -1, -1):
            s = other(turn)
            give_back(s, acc[s])

    w_copy.wait()
    for j in range(local_groups * cores):
        block = abuf.at[j]
        pltpu.make_async_copy(block, block, a_recv.at[j]).wait()

    half = rows // cores
    attended = jnp.concatenate([abuf[j] for j in range(local_groups * cores)], axis=1)

    def p_copy(j):
        return pltpu.make_async_remote_copy(
            src_ref=sendbuf.at[j, pl.ds(pl.multiple_of(partner * half, half), half), :],
            dst_ref=rbuf.at[j],
            send_sem=p_send.at[j],
            recv_sem=p_recv.at[j],
            device_id=(place, partner),
            device_id_type=MESH,
        )

    for j in range(blocks):
        product = jnp.dot(
            attended, wbuf[:, j * width : (j + 1) * width], preferred_element_type=jnp.float32
        )
        sendbuf[j] = product.astype(jnp.bfloat16)
        p_copy(j).start()
        part[j] = product
    for j in range(blocks):
        p_copy(j).wait_recv()
        mine = part[j, pl.ds(pl.multiple_of(core * half, half), half), :]
        out_ref[:, j * width : (j + 1) * width] = (mine + rbuf[j].astype(jnp.float32)).astype(
            out_ref.dtype
        )

    for j in range(blocks):
        p_copy(j).wait_send()
    for s in range(members):

        @pl.when(jnp.logical_not(a_is_own(s)))
        def _():
            a_copy(s).wait_send()

    for l in range(local_groups):
        for e in range(cores):

            @pl.when(jnp.logical_not(is_own(l, e)))
            def _():
                q_copy(l, e).wait_send()
                kv_copy(l, e).wait_send()

    def drain(index, none):
        fwd_copy(index).wait_send()

        @pl.when(plane < planes - 1)
        def _():
            z_copy(index).wait_send()

        return none

    lax.fori_loop(0, (plane + 1) * members, drain, 0)


def per_device(sizes, queries, keys, values, tile_mask, out_weight):
    seq_size, cores = sizes
    rows = queries.shape[0]
    local_groups = keys.shape[1] // HD
    group = queries.shape[1] // HD // local_groups
    members = local_groups * cores
    planes = seq_size // members
    heads = group // cores
    tile = rows * seq_size // tile_mask.shape[0]
    columns = out_weight.shape[1]
    wide = -(-tile_mask.shape[0] // HD) * HD
    width = math.gcd(columns, 512)
    blocks = columns // width
    dims = (planes, members, cores, local_groups, rows, heads, tile, blocks, width)
    bf16, f32 = jnp.bfloat16, jnp.float32
    DMA = pltpu.SemaphoreType.DMA
    any_spec = pl.BlockSpec(memory_space=pltpu.HBM)
    vmem_spec = pl.BlockSpec(memory_space=pltpu.VMEM)
    return pl.pallas_call(
        functools.partial(fused_kernel, dims),
        out_shape=jax.ShapeDtypeStruct((rows // cores, columns), bf16),
        in_specs=[any_spec] * 5,
        out_specs=vmem_spec,
        scratch_shapes=[
            pltpu.VMEM(tile_mask.shape, jnp.int32),
            pltpu.VMEM(queries.shape, bf16),
            pltpu.VMEM((2,) + keys.shape, bf16),
            pltpu.VMEM((members, rows, heads * HD), bf16),
            pltpu.VMEM((members, heads * rows, HD + wide), bf16),
            pltpu.VMEM((2, seq_size * rows, HD), bf16),
            pltpu.VMEM((members * rows, wide), bf16),
            pltpu.VMEM(out_weight.shape, bf16),
            pltpu.VMEM((members, heads * rows, 1), f32),
            pltpu.VMEM((members, heads * rows, 2 * HD), f32),
            pltpu.VMEM((members, rows, heads * HD), bf16),
            pltpu.VMEM((members, rows, heads * HD), bf16),
            pltpu.VMEM((blocks, rows, width), f32),
            pltpu.VMEM((blocks, rows, width), bf16),
            pltpu.VMEM((blocks, rows // cores, width), bf16),
            DMA((4,)),
            DMA,
            DMA((local_groups, 2)),
            DMA((seq_size,)),
            DMA((local_groups, cores)),
            DMA((members,)),
            DMA((seq_size,)),
            DMA((seq_size,)),
            DMA((seq_size,)),
            DMA((members,)),
            DMA((members,)),
            DMA((blocks,)),
            DMA((blocks,)),
        ],
        compiler_params=pltpu.CompilerParams(
            collective_id=0, has_side_effects=True, vmem_limit_bytes=60 << 20
        ),
        name="attend_project",
    )(queries, keys, values, tile_mask, out_weight)


def solution(mesh):
    placed = (P("seq", "head"), P("seq", "head"), P("seq", "head"), P(), P("head", None))
    sizes = (mesh.shape["seq"], mesh.shape["head"])
    return jax.shard_map(
        functools.partial(per_device, sizes),
        mesh=mesh,
        in_specs=placed,
        out_specs=P(("seq", "head"), None),
        check_vma=False,
    )
```

```python
import functools
import math

import jax
import jax.numpy as jnp
from jax import lax
from jax.experimental import pallas as pl
from jax.experimental.pallas import tpu as pltpu
from jax.sharding import PartitionSpec as P

HD = 128
MASK_FLOOR = -1e30
MESH = pl.DeviceIdType.MESH


def fused_kernel(
    dims,
    q_hbm, k_hbm, v_hbm, mask_hbm, w_hbm,
    out_ref,
    mask_ref, q_in, kv_in, qbuf, qext, kvbuf, spread, wbuf, best, acc, attbuf, abuf, part, sendbuf, rbuf,
    load_sem, w_sem, kv_send, kv_recv, q_send, q_recv, z_send, fwd_send, fwd_recv,
    a_send, a_recv, p_send, p_recv,
):
    planes, members, cores, local_groups, rows, heads, tile, blocks, width = dims
    place = lax.axis_index("seq")
    core = lax.axis_index("head")
    plane = place // members
    member = lax.rem(place, members)
    partner = 1 - core
    home = member // local_groups
    chunk = members * rows
    hw = heads * HD

    loads = [
        pltpu.make_async_copy(k_hbm, kv_in.at[0], load_sem.at[0]),
        pltpu.make_async_copy(v_hbm, kv_in.at[1], load_sem.at[1]),
        pltpu.make_async_copy(q_hbm, q_in, load_sem.at[2]),
        pltpu.make_async_copy(mask_hbm, mask_ref, load_sem.at[3]),
    ]
    for load in loads:
        load.start()

    barrier = pltpu.get_barrier_semaphore()

    def greet(seq_to, head_to):
        pl.semaphore_signal(barrier, inc=1, device_id=(seq_to, head_to), device_id_type=MESH)

    for shift in range(1, members * cores):
        peer = lax.rem(member * cores + core + shift, members * cores)
        greet(plane * members + peer // cores, lax.rem(peer, cores))

    @pl.when(plane < planes - 1)
    def _():
        greet(place + members, core)

    @pl.when(plane > 0)
    def _():
        greet(place - members, core)

    w_copy = pltpu.make_async_copy(w_hbm, wbuf, w_sem)

    for load in loads[:2]:
        load.wait()
    pl.semaphore_wait(
        barrier,
        members * cores - 1 + jnp.minimum(plane, 1) + jnp.minimum(planes - 1 - plane, 1),
    )

    def is_own(l, kind):
        return (core * local_groups + l == member) & (core == kind)

    def block_at(index):
        return pl.ds(pl.multiple_of(index * rows, rows), rows)

    def kv_copy(l, kind):
        return pltpu.make_async_remote_copy(
            src_ref=kv_in.at[kind, :, pl.ds(l * HD, HD)],
            dst_ref=kvbuf.at[kind, block_at(place), :],
            send_sem=kv_send.at[l, kind],
            recv_sem=kv_recv.at[place],
            device_id=(plane * members + core * local_groups + l, kind),
            device_id_type=MESH,
        )

    for l in range(local_groups):
        for kind in range(2):

            @pl.when(is_own(l, kind))
            def _():
                pltpu.make_async_copy(
                    kv_in.at[kind, :, pl.ds(l * HD, HD)],
                    kvbuf.at[kind, block_at(place), :],
                    kv_recv.at[place],
                ).start()

            @pl.when(jnp.logical_not(is_own(l, kind)))
            def _():
                kv_copy(l, kind).start()

    for load in loads[2:]:
        load.wait()

    def q_copy(l, e):
        return pltpu.make_async_remote_copy(
            src_ref=q_in.at[:, pl.ds((l * cores + e) * hw, hw)],
            dst_ref=qbuf.at[member],
            send_sem=q_send.at[l, e],
            recv_sem=q_recv.at[member],
            device_id=(plane * members + core * local_groups + l, e),
            device_id_type=MESH,
        )

    for l in range(local_groups):
        for e in range(cores):

            @pl.when(is_own(l, e))
            def _():
                pltpu.make_async_copy(
                    q_in.at[:, pl.ds((l * cores + e) * hw, hw)], qbuf.at[member], q_recv.at[member]
                ).start()

            @pl.when(jnp.logical_not(is_own(l, e)))
            def _():
                q_copy(l, e).start()

    w_copy.start()

    def z_copy(index):
        return pltpu.make_async_remote_copy(
            src_ref=kvbuf.at[core, block_at(index), :],
            dst_ref=kvbuf.at[core, block_at(index), :],
            send_sem=z_send.at[index],
            recv_sem=kv_recv.at[index],
            device_id=(place + members, core),
            device_id_type=MESH,
        )

    def fwd_copy(index):
        return pltpu.make_async_remote_copy(
            src_ref=kvbuf.at[core, block_at(index), :],
            dst_ref=kvbuf.at[core, block_at(index), :],
            send_sem=fwd_send.at[index],
            recv_sem=fwd_recv.at[index],
            device_id=(place, partner),
            device_id_type=MESH,
        )

    def other(turn):
        across = lax.rem(member // 2 + turn // 2, members // 2) * 2
        return across + lax.rem(lax.rem(member, 2) + turn % 2, 2)

    def relay(kc, turn):
        index = kc * members + other(turn)
        block = kvbuf.at[core, block_at(index), :]
        pltpu.make_async_copy(block, block, kv_recv.at[index]).wait()

        @pl.when(plane < planes - 1)
        def _():
            z_copy(index).start()

        fwd_copy(index).start()

    def settle(kc):
        for s in range(members):
            block = kvbuf.at[partner, block_at(kc * members + s), :]
            pltpu.make_async_copy(block, block, fwd_recv.at[kc * members + s]).wait()
        key_at = kc * chunk + lax.broadcasted_iota(jnp.int32, (chunk, wide), 0)
        tile_from = lax.broadcasted_iota(jnp.int32, (chunk, wide), 1) * tile
        inside = (key_at >= tile_from) & (key_at < tile_from + tile)
        spread[...] = jnp.where(inside, 1.0, 0.0).astype(jnp.bfloat16)

    unit = math.log2(math.e) / math.sqrt(HD)

    def attend(kc, parts, first):
        base = pl.multiple_of(kc * chunk, chunk)
        olds = [None if first else (best[s], acc[s]) for s in parts]
        news = []
        for s, old in zip(parts, olds):
            keys_here = (s + 1) * rows if first else chunk
            k_part = kvbuf[0, pl.ds(base, keys_here), :]
            k_wide = jnp.concatenate([k_part, spread[:keys_here, :]], axis=1)
            v_part = kvbuf[1, pl.ds(base, keys_here), :]
            v_wide = jnp.concatenate([v_part, jnp.ones_like(v_part)], axis=1)
            scores = lax.dot_general(
                qext[s], k_wide, (((1,), (1,)), ((), ())), preferred_element_type=jnp.float32
            )
            if first:
                r = s * rows + lax.broadcasted_iota(jnp.int32, (rows, keys_here), 0)
                u = lax.broadcasted_iota(jnp.int32, (rows, keys_here), 1)
                later = jnp.where(u <= r, 0.0, MASK_FLOOR)
                scores = scores + jnp.concatenate([later] * heads, axis=0)
            top = jnp.max(scores, axis=1, keepdims=True)
            if not first:
                top = jnp.maximum(old[0], top)
            weights = jnp.exp2((scores - top) * unit).astype(jnp.bfloat16)
            product = jnp.dot(weights, v_wide, preferred_element_type=jnp.float32)
            if not first:
                product = old[1] * jnp.exp2((old[0] - top) * unit) + product
            news.append((top, product))
        for s, new in zip(parts, news):
            best[s] = new[0]
            acc[s] = new[1]
        return news

    slot = lax.rem(member, local_groups) * cores + core

    def a_copy(s):
        return pltpu.make_async_remote_copy(
            src_ref=attbuf.at[s],
            dst_ref=abuf.at[slot],
            send_sem=a_send.at[s],
            recv_sem=a_recv.at[slot],
            device_id=(plane * members + s, home),
            device_id_type=MESH,
        )

    def a_is_own(s):
        return (member == s) & (core == home)

    def give_back(s, total):
        for h in range(heads):
            mine = total[h * rows : (h + 1) * rows, :]
            attbuf[s, :, h * HD : (h + 1) * HD] = (mine[:, :HD] / mine[:, HD:]).astype(jnp.bfloat16)

        @pl.when(a_is_own(s))
        def _():
            pltpu.make_async_copy(attbuf.at[s], abuf.at[slot], a_recv.at[slot]).start()

        @pl.when(jnp.logical_not(a_is_own(s)))
        def _():
            a_copy(s).start()

    for t in range(members):
        relay(plane, t)

    @pl.when(plane >= 1)
    def _():
        for t in range(members):
            relay(plane - 1, t)

    tiles = mask_ref.shape[0]
    wide = qext.shape[2] - HD
    row_at = plane * chunk + lax.broadcasted_iota(jnp.int32, (chunk, tiles), 0)
    tile_at = lax.broadcasted_iota(jnp.int32, (chunk, tiles), 1) * tile
    pick = jnp.where((row_at >= tile_at) & (row_at < tile_at + tile), 1.0, 0.0).astype(jnp.bfloat16)
    closed = jnp.where(mask_ref[...] > 0, 0.0, 1.0).astype(jnp.bfloat16)
    if wide > tiles:
        closed = jnp.concatenate([closed, jnp.zeros((tiles, wide - tiles), jnp.bfloat16)], axis=1)
    shut = jnp.dot(pick, closed, preferred_element_type=jnp.float32)
    floor = jnp.where(shut > 0.5, MASK_FLOOR, 0.0).astype(jnp.bfloat16)
    for s in range(members):
        for h in range(heads):
            qext[s, h * rows : (h + 1) * rows, HD:] = floor[s * rows : (s + 1) * rows, :]

    ahead = jnp.where(plane < planes - 1, 2, 1)
    settle(plane)
    for pair in range(0, members, 2):

        @pl.when((plane >= 2) & (plane < planes - 1))
        def _():
            relay(plane - 2, pair)
            relay(plane - 2, pair + 1)

        for s in (pair, pair + 1):
            block = qbuf.at[s]
            pltpu.make_async_copy(block, block, q_recv.at[s]).wait()
            for h in range(heads):
                qext[s, h * rows : (h + 1) * rows, :HD] = qbuf[s, :, h * HD : (h + 1) * HD]
        attend(plane, (pair, pair + 1), True)

    def below(step, none):
        settle(plane - step)
        for pair in range(0, members, 2):

            @pl.when(step + ahead <= plane)
            def _():
                relay(plane - step - ahead, pair)
                relay(plane - step - ahead, pair + 1)

            attend(plane - step, (pair, pair + 1), False)
        return none

    lax.fori_loop(1, plane, below, 0)

    @pl.when(plane >= 1)
    def _():
        settle(0)
        for pair in range(members // 2 - 1, -1, -1):
            parts = (other(2 * pair + 1), other(2 * pair))
            news = attend(0, parts, False)
            for s, new in zip(parts, news):
                give_back(s, new[1])

    @pl.when(plane == 0)
    def _():
        for turn in range(members - 1, -1, -1):
            s = other(turn)
            give_back(s, acc[s])

    w_copy.wait()
    half = rows // cores
    def p_copy(j):
        return pltpu.make_async_remote_copy(
            src_ref=sendbuf.at[j, pl.ds(pl.multiple_of(partner * half, half), half), :],
            dst_ref=rbuf.at[j],
            send_sem=p_send.at[j],
            recv_sem=p_recv.at[j],
            device_id=(place, partner),
            device_id_type=MESH,
        )

    for l in range(local_groups):
        for e in range(cores):
            block = abuf.at[l * cores + e]
            pltpu.make_async_copy(block, block, a_recv.at[l * cores + e]).wait()
        attended = jnp.concatenate([abuf[l * cores + e] for e in range(cores)], axis=1)
        depth = cores * hw
        for j in range(blocks):
            product = jnp.dot(
                attended,
                wbuf[l * depth : (l + 1) * depth, j * width : (j + 1) * width],
                preferred_element_type=jnp.float32,
            )
            if l > 0:
                product = part[j] + product
            if l == local_groups - 1:
                sendbuf[j] = product.astype(jnp.bfloat16)
                p_copy(j).start()
            part[j] = product
    for j in range(blocks):
        p_copy(j).wait_recv()
        mine = part[j, pl.ds(pl.multiple_of(core * half, half), half), :]
        out_ref[:, j * width : (j + 1) * width] = (mine + rbuf[j].astype(jnp.float32)).astype(
            out_ref.dtype
        )

    for j in range(blocks):
        p_copy(j).wait_send()
    for s in range(members):

        @pl.when(jnp.logical_not(a_is_own(s)))
        def _():
            a_copy(s).wait_send()

    for l in range(local_groups):
        for e in range(cores):

            @pl.when(jnp.logical_not(is_own(l, e)))
            def _():
                q_copy(l, e).wait_send()
                kv_copy(l, e).wait_send()

    def drain(index, none):
        fwd_copy(index).wait_send()

        @pl.when(plane < planes - 1)
        def _():
            z_copy(index).wait_send()

        return none

    lax.fori_loop(0, (plane + 1) * members, drain, 0)


def per_device(sizes, queries, keys, values, tile_mask, out_weight):
    seq_size, cores = sizes
    rows = queries.shape[0]
    local_groups = keys.shape[1] // HD
    group = queries.shape[1] // HD // local_groups
    members = local_groups * cores
    planes = seq_size // members
    heads = group // cores
    tile = rows * seq_size // tile_mask.shape[0]
    columns = out_weight.shape[1]
    wide = -(-tile_mask.shape[0] // HD) * HD
    width = math.gcd(columns, 2048)
    blocks = columns // width
    dims = (planes, members, cores, local_groups, rows, heads, tile, blocks, width)
    bf16, f32 = jnp.bfloat16, jnp.float32
    DMA = pltpu.SemaphoreType.DMA
    any_spec = pl.BlockSpec(memory_space=pltpu.HBM)
    vmem_spec = pl.BlockSpec(memory_space=pltpu.VMEM)
    return pl.pallas_call(
        functools.partial(fused_kernel, dims),
        out_shape=jax.ShapeDtypeStruct((rows // cores, columns), bf16),
        in_specs=[any_spec] * 5,
        out_specs=vmem_spec,
        scratch_shapes=[
            pltpu.VMEM(tile_mask.shape, jnp.int32),
            pltpu.VMEM(queries.shape, bf16),
            pltpu.VMEM((2,) + keys.shape, bf16),
            pltpu.VMEM((members, rows, heads * HD), bf16),
            pltpu.VMEM((members, heads * rows, HD + wide), bf16),
            pltpu.VMEM((2, seq_size * rows, HD), bf16),
            pltpu.VMEM((members * rows, wide), bf16),
            pltpu.VMEM(out_weight.shape, bf16),
            pltpu.VMEM((members, heads * rows, 1), f32),
            pltpu.VMEM((members, heads * rows, 2 * HD), f32),
            pltpu.VMEM((members, rows, heads * HD), bf16),
            pltpu.VMEM((members, rows, heads * HD), bf16),
            pltpu.VMEM((blocks, rows, width), f32),
            pltpu.VMEM((blocks, rows, width), bf16),
            pltpu.VMEM((blocks, rows // cores, width), bf16),
            DMA((4,)),
            DMA,
            DMA((local_groups, 2)),
            DMA((seq_size,)),
            DMA((local_groups, cores)),
            DMA((members,)),
            DMA((seq_size,)),
            DMA((seq_size,)),
            DMA((seq_size,)),
            DMA((members,)),
            DMA((members,)),
            DMA((blocks,)),
            DMA((blocks,)),
        ],
        compiler_params=pltpu.CompilerParams(
            collective_id=0, has_side_effects=True, vmem_limit_bytes=60 << 20
        ),
        name="attend_project",
    )(queries, keys, values, tile_mask, out_weight)


def solution(mesh):
    placed = (P("seq", "head"), P("seq", "head"), P("seq", "head"), P(), P("head", None))
    sizes = (mesh.shape["seq"], mesh.shape["head"])
    return jax.shard_map(
        functools.partial(per_device, sizes),
        mesh=mesh,
        in_specs=placed,
        out_specs=P(("seq", "head"), None),
        check_vma=False,
    )
```
